256 devices in a mesh: row: 8 (over z_hi, y), col: 32 (over z_lo, x, core).
Axes of the slice: x: 4, y: 4, z: 8 (z_hi: 2, z_lo: 4; z = z_hi * 4 + z_lo), core: 2. Of those that a mesh axis runs over, the one named last changes fastest.
Arguments:
- tokens: bfloat16 [4096, 1024], P(('row', 'col')), may hold values from -6 to 6
- grad_out: bfloat16 [4096, 1024], P(('row', 'col')), may hold values from -1.1953125 to 1.1953125
- gains: float32 [2, 1024], replicated, may hold values from 0.1 to 1.9
- flat_in: bfloat16 [32768, 1024], P(('row', 'col')), may hold values from -0.1875 to 0.1875
- flat_out: bfloat16 [32768, 1024], P(('row', 'col')), may hold values from -0.03125 to 0.03125
- flat_moment: float32 [2, 32768, 1024], P(None, ('row', 'col')), may hold values from -3 to 3
- flat_second: float32 [2, 32768, 1024], P(None, ('row', 'col')), may hold values from 0.05 to 2
- tile_in: bfloat16 [32, 24, 64, 1024], P('col', 'row'), may hold values from -0.1875 to 0.1875
- tile_out: bfloat16 [32, 24, 64, 1024], P('col', 'row'), may hold values from -0.03125 to 0.03125
- tile_moment: float32 [2, 32, 24, 64, 1024], P(None, 'col', 'row'), may hold values from -3 to 3
- tile_second: float32 [2, 32, 24, 64, 1024], P(None, 'col', 'row'), may hold values from 0.05 to 2
- owners: int32 [2, 32, 16], P(None, 'col'), may hold values from 0 to 7, as said below
Outputs:
- hidden_out: bfloat16 [4096, 1024], P(('row', 'col'))
- grad_tokens: bfloat16 [4096, 1024], P(('row', 'col'))
- new_flat_in: bfloat16 [32768, 1024], P(('row', 'col'))
- new_flat_out: bfloat16 [32768, 1024], P(('row', 'col'))
- new_flat_moment: float32 [2, 32768, 1024], P(None, ('row', 'col'))
- new_flat_second: float32 [2, 32768, 1024], P(None, ('row', 'col'))
- new_tile_in: bfloat16 [32, 24, 64, 1024], P('col', 'row')
- new_tile_out: bfloat16 [32, 24, 64, 1024], P('col', 'row')
- new_tile_moment: float32 [2, 32, 24, 64, 1024], P(None, 'col', 'row')
- new_tile_second: float32 [2, 32, 24, 64, 1024], P(None, 'col', 'row')
The draws below stay inside these ranges and needn't reach their ends.
Inputs may be any that keep to these rules, and one draw needn't show every extreme that they name: `owners`: for each matrix and column block, entry k names the row that owns tile k; each row owns at most 3 tiles of a block and matrix, and in each block and matrix some row owns exactly 3.
All inputs are finite; a program needn't handle non-finite values.
Results may differ from the reference program's by a relative error of at most 0.029.
Values may be sent and summed in bfloat16 or wider, within the bound.
No kernel may reach another device: no remote copies, remote signals or barrier semaphores. Data moves between devices by JAX's collectives and lax.ppermute only.
A program may use at most 128 MiB of HBM per device.

```python
import math
import jax
import jax.numpy as jnp
from jax import lax

D = 1024
FF = 32768
OWN_CAP = 3
TOKENS = 4096
GROUP_TOK = 512
BLOCK = 1024
TILES = 16
TILE_ROWS = 64
N_ROW = 8
N_COL = 32


def draw_owners(key, part):
    owner_pool = jnp.repeat(jnp.arange(N_ROW, dtype=jnp.int32), OWN_CAP)

    def one_block(sub_key):
        key_full, key_pick, key_order = jax.random.split(sub_key, 3)
        favored = jax.random.randint(key_full, (), 0, N_ROW, dtype=jnp.int32)
        scores = jax.random.permutation(key_pick, N_ROW * OWN_CAP).astype(jnp.int32) + jnp.where(owner_pool == favored, N_ROW * OWN_CAP, 0).astype(jnp.int32)
        picked = jnp.argsort(-scores, stable=True)[:2 * N_ROW]
        chosen = owner_pool[picked]
        return chosen[jax.random.permutation(key_order, 2 * N_ROW)]
    block_keys = jax.random.split(jax.random.fold_in(key, 17), 2 * N_COL)
    return jax.vmap(one_block)(block_keys).reshape(2, N_COL, 2 * N_ROW).astype(jnp.int32)


def block_levels(own_key, dims, cuts, least, high):
    factor_of, own = 1.0, jax.random.fold_in(own_key, 6)
    for position, shards_of in cuts:
        draws = jnp.exp(jax.random.uniform(jax.random.fold_in(own, position), (shards_of,), jnp.float32, least / len(cuts), high / len(cuts)))
        factor_of = factor_of * jnp.repeat(draws, dims[position] // shards_of).reshape([-1 if axis == position else 1 for axis in range(len(dims))])
    return factor_of


def bell_draw(rng, dims, deviation, reach, cuts=(), kind=jnp.bfloat16):
    drawn = jax.random.normal(rng, dims, jnp.float32) * deviation
    if len(cuts) > 0:
        drawn = block_levels(rng, dims, cuts, -0.22, 0.18) * drawn
    return jnp.clip(drawn, min=-reach, max=reach).astype(kind)


def setup_inputs(seed: int = 0) -> dict:
    streams_of = jax.random.split(jax.random.key(seed), 13)
    tokens = bell_draw(streams_of[0], (TOKENS, D), 1.0, 6.0, ((0, 256),))
    grad_out = bell_draw(streams_of[1], (TOKENS, D), 0.2, 1.1953125, ((0, 256),))
    gains = jnp.clip(1.0 + 0.18 * jax.random.normal(streams_of[2], (2, D), jnp.float32), 0.1, 1.9)
    flat_in = bell_draw(streams_of[3], (D * N_COL, BLOCK), D ** -0.5, 0.1875, ((0, 256),))
    flat_out = bell_draw(streams_of[4], (D * N_COL, BLOCK), FF ** -0.5, 0.03125, ((0, 256),))
    flat_moment = bell_draw(streams_of[5], (2, D * N_COL, BLOCK), 0.5, 3.0, ((1, 256),), jnp.float32)
    flat_second = jnp.clip(jnp.exp(math.log(2.0) - 3.6888794 * jax.random.uniform(streams_of[6], (2, D * N_COL, BLOCK), jnp.float32) ** block_levels(streams_of[6], (2, D * N_COL, BLOCK), ((1, 256),), -0.2, 0.2)), 0.05, 2.0)
    tile_in = bell_draw(streams_of[7], (N_COL, N_ROW * OWN_CAP, TILE_ROWS, BLOCK), D ** -0.5, 0.1875, ((0, 32), (1, 8)))
    tile_out = bell_draw(streams_of[8], (N_COL, N_ROW * OWN_CAP, TILE_ROWS, BLOCK), FF ** -0.5, 0.03125, ((0, 32), (1, 8)))
    tile_moment = bell_draw(streams_of[9], (2, N_COL, N_ROW * OWN_CAP, TILE_ROWS, BLOCK), 0.5, 3.0, ((1, 32), (2, 8)), jnp.float32)
    tile_second = jnp.clip(jnp.exp(math.log(2.0) - 3.6888794 * jax.random.uniform(streams_of[10], (2, N_COL, N_ROW * OWN_CAP, TILE_ROWS, BLOCK), jnp.float32) ** block_levels(streams_of[10], (2, N_COL, N_ROW * OWN_CAP, TILE_ROWS, BLOCK), ((1, 32), (2, 8)), -0.2, 0.2)), 0.05, 2.0)
    owners = draw_owners(jax.random.fold_in(streams_of[12], 71), 0)
    return dict(tokens=tokens, grad_out=grad_out, gains=gains, flat_in=flat_in, flat_out=flat_out, flat_moment=flat_moment, flat_second=flat_second, tile_in=tile_in, tile_out=tile_out, tile_moment=tile_moment, tile_second=tile_second, owners=owners)


norm_eps = 1e-06
beta_one = 0.9
beta_two = 0.95
learn_rate = 0.002
decay_rate = 0.1
adam_eps = 1e-08
gelu_coef = 0.7978845608

def gelu_value(hidden):
    tanh_term = jnp.tanh(gelu_coef * (hidden + 0.044715 * hidden * hidden * hidden))
    return 0.5 * hidden * (1.0 + tanh_term)

def gelu_slope(hidden):
    tanh_term = jnp.tanh(gelu_coef * (hidden + 0.044715 * hidden * hidden * hidden))
    return 0.5 * (1.0 + tanh_term) + 0.5 * hidden * (1.0 - tanh_term * tanh_term) * gelu_coef * (1.0 + 0.134145 * hidden * hidden)

def adam_update(weight, gradient, moment, second):
    new_moment = beta_one * moment + (1.0 - beta_one) * gradient
    new_second = beta_two * second + (1.0 - beta_two) * gradient * gradient
    weight_float = weight.astype(jnp.float32)
    stepped = weight_float - learn_rate * (new_moment / (jnp.sqrt(new_second) + adam_eps) + decay_rate * weight_float)
    return (stepped.astype(jnp.bfloat16), new_moment, new_second)

def slot_tables(owner_rows, slot_cap, row_total):
    tile_count = owner_rows.shape[-1]
    positions = jnp.arange(tile_count, dtype=jnp.int32)
    same_owner = owner_rows[..., :, None] == owner_rows[..., None, :]
    earlier = positions[None, :] < positions[:, None]
    tile_rank = lax.optimization_barrier(jnp.sum(jnp.where(same_owner & earlier, 1, 0), axis=-1)).astype(jnp.int32)
    slot_dest = (owner_rows * slot_cap + tile_rank).astype(jnp.int32)
    slot_ids = jnp.arange(row_total * slot_cap, dtype=jnp.int32)
    matches = slot_dest[..., None, :] == slot_ids[:, None]
    slot_tile = lax.optimization_barrier(jnp.sum(jnp.where(matches, positions, 0), axis=-1)).astype(jnp.int32)
    slot_live = jnp.any(matches, axis=-1)
    return (slot_dest, slot_tile, slot_live)

def layer_forward(layer_in, gain_vec, w_in, w_out):
    tok_float = layer_in.astype(jnp.float32)
    inv_rms = lax.rsqrt(lax.optimization_barrier(jnp.mean(tok_float * tok_float, axis=1, keepdims=True)) + norm_eps)
    normed = (tok_float * inv_rms * gain_vec).astype(jnp.bfloat16)
    hidden = jnp.dot(normed, w_in, preferred_element_type=jnp.float32)
    activated = gelu_value(hidden).astype(jnp.bfloat16)
    mixed_sum = lax.dot_general(activated, w_out, (((1,), (1,)), ((), ())), preferred_element_type=jnp.float32)
    return ((tok_float + mixed_sum).astype(jnp.bfloat16), (tok_float, inv_rms, normed, hidden, activated))

def group_sums(left_rows, right_rows):
    left_groups = left_rows.reshape(N_ROW, GROUP_TOK, left_rows.shape[1])
    right_groups = right_rows.reshape(N_ROW, GROUP_TOK, right_rows.shape[1])

    def add_group(running, operands):
        product = lax.dot_general(operands[0], operands[1], (((0,), (0,)), ((), ())), preferred_element_type=jnp.float32)
        rounded = lax.optimization_barrier(product.astype(jnp.bfloat16))
        return (running + rounded.astype(jnp.float32), None)
    start_sum = jnp.zeros((left_rows.shape[1], right_rows.shape[1]), jnp.float32)
    running, unused = lax.scan(add_group, start_sum, (left_groups, right_groups))
    return running

def layer_backward(cotangent, gain_vec, w_in, w_out, saved_state):
    tok_float, inv_rms, normed, hidden, activated = saved_state
    d_act = jnp.dot(cotangent, w_out, preferred_element_type=jnp.float32)
    d_hidden = (d_act * gelu_slope(hidden)).astype(jnp.bfloat16)
    d_normed = lax.dot_general(d_hidden, w_in, (((1,), (1,)), ((), ())), preferred_element_type=jnp.float32)
    gated = d_normed * gain_vec
    tok_grad = cotangent.astype(jnp.float32) + inv_rms * gated - tok_float * inv_rms * inv_rms * inv_rms * lax.optimization_barrier(jnp.mean(tok_float * gated, axis=1, keepdims=True))
    grad_in = group_sums(normed, d_hidden)
    grad_wout = group_sums(cotangent, activated)
    return (tok_grad.astype(jnp.bfloat16), grad_in, grad_wout)

def assemble(slot_data, slot_dest_m):
    tile_data = jnp.take_along_axis(slot_data, slot_dest_m[:, :, None, None], axis=1)
    return tile_data.transpose(1, 2, 0, 3).reshape(D, FF)

def tiled_update(slot_data, gradient, moment, second, slot_tile_m, slot_live_m):
    grad_tiles = gradient.reshape(TILES, TILE_ROWS, N_COL, BLOCK).transpose(2, 0, 1, 3)
    grad_slots = jnp.take_along_axis(grad_tiles, slot_tile_m[:, :, None, None], axis=1)
    new_weight, new_moment, new_second = adam_update(slot_data, grad_slots, moment, second)
    live_mask = slot_live_m[:, :, None, None]
    return (jnp.where(live_mask, new_weight, slot_data), jnp.where(live_mask, new_moment, moment), jnp.where(live_mask, new_second, second))

def reference(tokens, grad_out, gains, flat_in, flat_out, flat_moment, flat_second, tile_in, tile_out, tile_moment, tile_second, owners):
    slot_dest, slot_tile, slot_live = slot_tables(owners, OWN_CAP, N_ROW)
    first_in = flat_in.reshape(D, FF)
    first_out = flat_out.reshape(D, FF)
    second_in = assemble(tile_in, slot_dest[0])
    second_out = assemble(tile_out, slot_dest[1])
    middle, saved_one = layer_forward(tokens, gains[0], first_in, first_out)
    hidden_out, saved_two = layer_forward(middle, gains[1], second_in, second_out)
    grad_mid, grad_in_two, grad_out_two = layer_backward(grad_out, gains[1], second_in, second_out, saved_two)
    grad_tokens, grad_in_one, grad_out_one = layer_backward(grad_mid, gains[0], first_in, first_out, saved_one)
    new_flat_in, moment_in, second_in_f = adam_update(flat_in, grad_in_one.reshape(D * N_COL, BLOCK), flat_moment[0], flat_second[0])
    new_flat_out, moment_out, second_out_f = adam_update(flat_out, grad_out_one.reshape(D * N_COL, BLOCK), flat_moment[1], flat_second[1])
    new_tile_in, tmoment_in, tsecond_in = tiled_update(tile_in, grad_in_two, tile_moment[0], tile_second[0], slot_tile[0], slot_live[0])
    new_tile_out, tmoment_out, tsecond_out = tiled_update(tile_out, grad_out_two, tile_moment[1], tile_second[1], slot_tile[1], slot_live[1])
    return (hidden_out, grad_tokens, new_flat_in, new_flat_out, jnp.stack([moment_in, moment_out]), jnp.stack([second_in_f, second_out_f]), new_tile_in, new_tile_out, jnp.stack([tmoment_in, tmoment_out]), jnp.stack([tsecond_in, tsecond_out]))
```

```python
import jax
import jax.numpy as jnp
from jax import lax
from jax.sharding import Mesh, PartitionSpec as P

norm_eps = 1e-06
beta_one = 0.9
beta_two = 0.95
learn_rate = 0.002
decay_rate = 0.1
adam_eps = 1e-08
gelu_coef = 0.7978845608


AXES = ("zh", "y", "zl", "x", "c")
PLANE = ("zh", "zl", "x", "c")


def from_ahead(value, axis, k):
    n = lax.axis_size(axis)
    return lax.ppermute(value, axis, [(s, (s - k) % n) for s in range(n)])


def to_ahead(value, axis, k):
    n = lax.axis_size(axis)
    return lax.ppermute(value, axis, [(s, (s + k) % n) for s in range(n)])


def gather_axis(value, axis):
    n = lax.axis_size(axis)
    return jnp.stack([value] + [from_ahead(value, axis, k) for k in range(1, n)])


def gather_plane(value):
    rows, width = value.shape
    for axis in ("zh", "zl", "x", "c"):
        value = gather_axis(value, axis)
        value = value.reshape(-1, width)
    return value


def scatter_axis(parts, axis):
    n = lax.axis_size(axis)
    total = parts[0].astype(jnp.float32)
    for k in range(1, n):
        total = total + to_ahead(parts[k].astype(jnp.bfloat16), axis, k).astype(jnp.float32)
    return total


def scatter_plane(value):
    width = value.shape[-1]
    for axis in ("c", "x", "zl", "zh"):
        n = lax.axis_size(axis)
        value = value.reshape(n, -1, width)
        value = scatter_axis([value[k] for k in range(n)], axis)
    return value


def rolled(value, shift):
    rows = value.shape[0]
    halves = value.reshape(rows, 2, 512)
    doubled = jnp.concatenate([halves, halves], axis=2)
    return lax.dynamic_slice_in_dim(doubled, shift * 128, 512, axis=2).reshape(rows, 1024)


def gelu_both(hidden):
    tanh_term = jnp.tanh(gelu_coef * (hidden + 0.044715 * hidden * hidden * hidden))
    value = 0.5 * hidden * (1.0 + tanh_term)
    slope = 0.5 * (1.0 + tanh_term) + 0.5 * hidden * (1.0 - tanh_term * tanh_term) * gelu_coef * (
        1.0 + 0.134145 * hidden * hidden
    )
    return (value.astype(jnp.bfloat16), slope)


def adam_update(weight, gradient, moment, second):
    new_moment = beta_one * moment + (1.0 - beta_one) * gradient
    new_second = beta_two * second + (1.0 - beta_two) * gradient * gradient
    weight_float = weight.astype(jnp.float32)
    stepped = weight_float - learn_rate * (
        new_moment / (jnp.sqrt(new_second) + adam_eps) + decay_rate * weight_float
    )
    return (stepped.astype(jnp.bfloat16), new_moment, new_second)


def dot(a, b):
    return jnp.dot(a, b, preferred_element_type=jnp.float32)


def dot_t(a, b):
    return lax.dot_general(a, b, (((1,), (1,)), ((), ())), preferred_element_type=jnp.float32)


def t_dot(a, b):
    return lax.dot_general(a, b, (((0,), (0,)), ((), ())), preferred_element_type=jnp.float32)


def norm(layer_in, gain_vec):
    tok_float = layer_in.astype(jnp.float32)
    inv_rms = lax.rsqrt(jnp.mean(tok_float * tok_float, axis=1, keepdims=True) + norm_eps)
    return ((tok_float * inv_rms * gain_vec).astype(jnp.bfloat16), tok_float, inv_rms)


def norm_back(cotangent, d_normed, gain_vec, tok_float, inv_rms):
    gated = d_normed * gain_vec
    return (
        cotangent.astype(jnp.float32)
        + inv_rms * gated
        - tok_float
        * inv_rms
        * inv_rms
        * inv_rms
        * jnp.mean(tok_float * gated, axis=1, keepdims=True)
    ).astype(jnp.bfloat16)


def flat_weights(flat):
    pieces = flat.reshape(4, 32, 2, 512).transpose(2, 1, 0, 3).reshape(64, 4, 512)
    banded = lax.all_to_all(pieces, PLANE, 0, 0, tiled=True).reshape(2, 128, 512)
    return gather_axis(banded, "y").transpose(1, 0, 2, 3).reshape(1024, 512)


def flat_gradient(grad):
    parts = grad.reshape(2, 4, 128, 512)
    summed = scatter_axis([parts[:, k] for k in range(4)], "y").astype(jnp.bfloat16)
    arrived = lax.all_to_all(summed.reshape(64, 4, 512), PLANE, 0, 0, tiled=True)
    return arrived.reshape(2, 32, 4, 512).transpose(2, 1, 0, 3).reshape(128, 1024)


def tile_weights(tile, places, zh):
    own = lax.dynamic_slice_in_dim(tile, zh * 512, 512, axis=2)
    other = lax.dynamic_slice_in_dim(tile, (1 - zh) * 512, 512, axis=2)
    pair = jnp.stack([own, from_ahead(other, "zh", 1)])
    slots = gather_axis(pair, "y").reshape(24, 64, 512)
    return jnp.take(slots, places, axis=0).reshape(1024, 512)


def tile_gradient(grad, slot_tile, slot_live, zh):
    tiles = grad.astype(jnp.bfloat16).reshape(16, 64, 512)
    slots = jnp.where(slot_live[:, None, None], jnp.take(tiles, slot_tile, axis=0), 0)
    slots = slots.reshape(4, 2, 3, 64, 512)
    summed = scatter_axis([slots[k] for k in range(4)], "y")
    own, other = (summed[0], to_ahead(summed[1].astype(jnp.bfloat16), "zh", 1).astype(jnp.float32))
    return jnp.where(
        zh == 0, jnp.concatenate([own, other], axis=2), jnp.concatenate([other, own], axis=2)
    )


def tile_places(owner_rows, zh, y):
    t = jnp.arange(16, dtype=jnp.int32)
    same = owner_rows[:, None] == owner_rows[None, :]
    rank = jnp.sum(jnp.where(same & (t[None, :] < t[:, None]), 1, 0), axis=-1)
    owner_zh, owner_y = (owner_rows // 4, owner_rows % 4)
    place = ((owner_y - y + 4) % 4) * 6 + ((owner_zh - zh + 2) % 2) * 3 + rank
    tile_of = (t // 8) * 8 + ((t // 2 + y) % 4) * 2 + t % 2
    places = jnp.sum(jnp.where(tile_of[:, None] == t[None, :], place[None, :], 0), axis=-1)
    slots = jnp.arange(24, dtype=jnp.int32)
    matches = slots[:, None] == places[None, :]
    return (
        places.astype(jnp.int32),
        jnp.sum(jnp.where(matches, t[None, :], 0), axis=-1).astype(jnp.int32),
        jnp.any(matches, axis=-1),
    )


def shards(
    tokens,
    grad_out,
    gains,
    flat_in,
    flat_out,
    flat_moment,
    flat_second,
    tile_in,
    tile_out,
    tile_moment,
    tile_second,
    owners,
):
    zh, y = (lax.axis_index("zh"), lax.axis_index("y"))
    tok = rolled(tokens, y)
    cot_two = rolled(grad_out, y)
    gain = rolled(gains, y)
    places_in, slot_in, live_in = tile_places(owners[0, 0], zh, y)
    places_out, slot_out, live_out = tile_places(owners[1, 0], zh, y)

    normed_one, tok_one, rms_one = norm(tok, gain[0])
    norm_all_one = gather_plane(normed_one)
    w_in_one = flat_weights(flat_in)
    w_out_one = flat_weights(flat_out)
    act_one, slope_one = gelu_both(dot(norm_all_one, w_in_one))
    middle = (tok_one + scatter_plane(dot_t(act_one, w_out_one))).astype(jnp.bfloat16)

    w_in_two = tile_weights(tile_in[0], places_in, zh)
    w_out_two = tile_weights(tile_out[0], places_out, zh)
    cot_all_two = gather_plane(cot_two)
    d_act_two = dot(cot_all_two, w_out_two)
    normed_two, tok_two, rms_two = norm(middle, gain[1])
    norm_all_two = gather_plane(normed_two)
    act_two, slope_two = gelu_both(dot(norm_all_two, w_in_two))
    d_hidden_two = (d_act_two * slope_two).astype(jnp.bfloat16)
    d_normed_two = scatter_plane(dot_t(d_hidden_two, w_in_two))
    grad_mid = norm_back(cot_two, d_normed_two, gain[1], tok_two, rms_two)
    cot_all_one = gather_plane(grad_mid)

    hidden_out = (tok_two + scatter_plane(dot_t(act_two, w_out_two))).astype(jnp.bfloat16)
    tile_grad_out = tile_gradient(t_dot(cot_all_two, act_two), slot_out, live_out, zh)
    tile_grad_in = tile_gradient(t_dot(norm_all_two, d_hidden_two), slot_in, live_in, zh)

    flat_grad_out = flat_gradient(t_dot(cot_all_one, act_one))
    d_hidden_one = (dot(cot_all_one, w_out_one) * slope_one).astype(jnp.bfloat16)
    flat_grad_in = flat_gradient(t_dot(norm_all_one, d_hidden_one))
    d_normed_one = scatter_plane(dot_t(d_hidden_one, w_in_one))
    grad_tokens = norm_back(grad_mid, d_normed_one, gain[0], tok_one, rms_one)

    new_flat_in, moment_in, second_in = adam_update(
        flat_in, flat_grad_in, flat_moment[0], flat_second[0]
    )
    new_flat_out, moment_out, second_out = adam_update(
        flat_out, flat_grad_out, flat_moment[1], flat_second[1]
    )
    tiles = []
    for m, (weight, gradient, live) in enumerate(
        ((tile_in[0], tile_grad_in, live_in), (tile_out[0], tile_grad_out, live_out))
    ):
        mask = live[:3][:, None, None]
        olds = (weight, tile_moment[m, 0], tile_second[m, 0])
        news = adam_update(weight, gradient, olds[1], olds[2])
        tiles.append([jnp.where(mask, new, old) for new, old in zip(news, olds)])
    back = (4 - y) % 4
    return (
        rolled(hidden_out, back),
        rolled(grad_tokens, back),
        new_flat_in,
        new_flat_out,
        jnp.stack([moment_in, moment_out]),
        jnp.stack([second_in, second_out]),
        tiles[0][0][None],
        tiles[1][0][None],
        jnp.stack([tiles[0][1], tiles[1][1]])[:, None],
        jnp.stack([tiles[0][2], tiles[1][2]])[:, None],
    )


def solution(mesh):
    fine = Mesh(mesh.devices.reshape(2, 4, 4, 4, 2), AXES)
    row, col = (("zh", "y"), ("zl", "x", "c"))
    both = row + col
    return jax.shard_map(
        shards,
        mesh=fine,
        in_specs=(
            P(both, None),
            P(both, None),
            P(),
            P(both, None),
            P(both, None),
            P(None, both, None),
            P(None, both, None),
            P(col, row, None, None),
            P(col, row, None, None),
            P(None, col, row, None, None),
            P(None, col, row, None, None),
            P(None, col, None),
        ),
        out_specs=(
            P(both, None),
            P(both, None),
            P(both, None),
            P(both, None),
            P(None, both, None),
            P(None, both, None),
            P(col, row, None, None),
            P(col, row, None, None),
            P(None, col, row, None, None),
            P(None, col, row, None, None),
        ),
        check_vma=False,
    )
```
